256 devices in a mesh: grp: 32 (over z, y_hi, core), seq: 8 (over y_lo, x).
Axes of the slice: x: 4, y: 4 (y_hi: 2, y_lo: 2; y = y_hi * 2 + y_lo), z: 8, core: 2. Of those that a mesh axis runs over, the one named last changes fastest.
Arguments:
- queries: bfloat16 [65536, 4096], P(('grp', 'seq')), may hold values from -8 to 8
- keys: bfloat16 [65536, 4096], P(('grp', 'seq')), may hold values from -6 to 6
- values: bfloat16 [65536, 4096], P(('grp', 'seq')), may hold values from -6 to 6
- global_pos: int32 [512], P(('grp', 'seq')), may hold values from 0 to 127
- layout: int32 [512, 32], P(('grp', 'seq')), may hold values from 0 to 511, all different within a row
Outputs:
- attended: bfloat16 [65536, 4096], P(('grp', 'seq'))
The draws below stay inside these ranges and needn't reach their ends.
Inputs may be any that keep to these rules, and one draw needn't show every extreme that they name: `layout`: each row lists 32 different block indices, and every block is listed by some row.
All inputs are finite; a program needn't handle non-finite values.
Results may differ from the reference program's by a relative error of at most 0.0042.
Values may be sent and summed in bfloat16 or wider, within the bound.
No kernel may reach another device: no remote copies, remote signals or barrier semaphores. Data moves between devices by JAX's collectives and lax.ppermute only.
A program may use at most 128 MiB of HBM per device.

```python
import math
import jax
import jax.numpy as jnp
from jax import lax

HEADS = 32
HEAD_DIM = 128
BLOCK = 128
LINKS = 32
WIDTH = 4096
SEQ = 65536
NBLK = 512


def draw_queries(key, part):
    base = jnp.clip(2.0 * jax.random.normal(jax.random.fold_in(key, 1), (SEQ, HEADS * HEAD_DIM), jnp.float32), -8.0, 8.0)
    return base.astype(jnp.bfloat16)


def draw_keys(key, part):
    base = jnp.clip(jax.random.normal(jax.random.fold_in(key, 2), (SEQ, HEADS * HEAD_DIM), jnp.float32), -6.0, 6.0)
    return base.astype(jnp.bfloat16)


def with_ends(entries, key, smallest, largest):
    longest = entries.shape.index(max(entries.shape))
    spots = []
    for shift in (0, 1):
        where = [jax.random.randint(jax.random.fold_in(key, axis), (), 0, length) for axis, length in enumerate(entries.shape)]
        where[longest] = (where[longest] + shift) % entries.shape[longest]
        spots.append(tuple(where))
    return entries.at[spots[0]].set(smallest).at[spots[1]].set(largest)


def shard_levels(key, extent, pieces, smallest, high):
    def one(dim, shards_of):
        heights = jax.random.uniform(jax.random.fold_in(jax.random.fold_in(key, 6), dim), (shards_of,), jnp.float32, smallest / len(pieces), high / len(pieces))
        return jnp.repeat(jnp.exp(heights), extent[dim] // shards_of).reshape((-1,) + (1,) * (len(extent) - dim - 1))

    factor_of = one(*pieces[0])
    for cut in pieces[1:]:
        factor_of = factor_of * one(*cut)
    return factor_of


def picks_of(key, rows, amount, top, lift):
    sequence = jax.random.permutation(jax.random.fold_in(key, 1), amount)
    boost = sequence
    for power in range(3):
        boost = boost * boost // amount
    boost = boost * lift // amount
    lots = jax.random.randint(jax.random.fold_in(key, 2), (rows, amount), 0, 4096) + boost
    sure = jax.random.permutation(jax.random.fold_in(key, 3), rows)[jnp.arange(amount) % rows]
    lots = jnp.where(jnp.arange(rows)[:, None] == sure[None, :], 1 << 14, lots)
    merit = lots * amount + jnp.arange(amount)
    return lax.top_k(merit.astype(jnp.int32), top)[1].astype(jnp.int32)


def noise(rng, dims, scale, reach, split=(), kind=jnp.bfloat16):
    values = jax.random.normal(rng, dims, jnp.float32) * scale
    if len(split) > 0:
        values = shard_levels(rng, dims, split, -0.22, 0.18) * values
    return jnp.clip(values, min=-reach, max=reach).astype(kind)


def setup_inputs(seed: int = 0) -> dict:
    seeds = jax.random.split(jax.random.key(seed), 6)
    return {
        "queries": draw_queries(jax.random.fold_in(seeds[5], 71), 0),
        "keys": draw_keys(jax.random.fold_in(seeds[5], 71), 0),
        "values": noise(seeds[2], (SEQ, WIDTH), 1.0, 6.0, ((0, 256),)),
        "global_pos": with_ends(jax.random.randint(seeds[3], (NBLK,), 0, BLOCK), jax.random.fold_in(seeds[3], 1), 0, BLOCK - 1).astype(jnp.int32),
        "layout": picks_of(seeds[4], NBLK, NBLK, LINKS, 0),
    }


def pooled(source, blocks_all):
    blocks = source.astype(jnp.float32).reshape(blocks_all, BLOCK, HEADS, HEAD_DIM).mean(axis=1)
    spread = lax.optimization_barrier(jnp.mean(blocks * blocks, axis=-1, keepdims=True))
    return (blocks / jnp.sqrt(spread + 1e-06)).reshape(blocks_all, HEADS * HEAD_DIM).astype(jnp.bfloat16)

def reference(queries, keys, values, global_pos, layout):
    score_scale = 1.0 / math.sqrt(HEAD_DIM)
    summary_keys = pooled(keys, NBLK).astype(jnp.float32).reshape(NBLK, HEADS, HEAD_DIM)
    summary_values = pooled(values, NBLK).astype(jnp.float32).reshape(NBLK, HEADS, HEAD_DIM)
    padding = jnp.zeros((BLOCK, HEADS * HEAD_DIM), jnp.bfloat16)
    padded_keys = jnp.concatenate([padding, keys, padding], axis=0)
    padded_values = jnp.concatenate([padding, values, padding], axis=0)
    block_ids = jnp.arange(NBLK, dtype=jnp.int32)

    def one_block(which):
        first_row = (which * BLOCK).astype(jnp.int32)
        query_rows = lax.dynamic_slice_in_dim(queries, first_row, BLOCK, 0).astype(jnp.float32).reshape(BLOCK, HEADS, HEAD_DIM)
        window_keys = lax.dynamic_slice_in_dim(padded_keys, first_row, 3 * BLOCK, 0).astype(jnp.float32).reshape(3 * BLOCK, HEADS, HEAD_DIM)
        window_values = lax.dynamic_slice_in_dim(padded_values, first_row, 3 * BLOCK, 0).astype(jnp.float32).reshape(3 * BLOCK, HEADS, HEAD_DIM)
        window_scores = jnp.einsum('qhd,khd->hqk', query_rows, window_keys) * score_scale
        key_block = jnp.arange(3 * BLOCK, dtype=jnp.int32) // BLOCK + which - 1
        inside = (key_block >= 0) & (key_block < NBLK)
        window_scores = jnp.where(inside[None, None, :], window_scores, -jnp.inf)
        summary_scores = jnp.einsum('qhd,jhd->hqj', query_rows, summary_keys) * score_scale
        listed = jnp.any(layout[which][:, None] == block_ids[None, :], axis=0)
        is_global = jnp.arange(BLOCK, dtype=jnp.int32) == global_pos[which]
        visible = listed[None, :] | is_global[:, None]
        summary_scores = jnp.where(visible[None, :, :], summary_scores, -jnp.inf)
        peak = jnp.maximum(lax.optimization_barrier(jnp.max(window_scores, axis=-1)), lax.optimization_barrier(jnp.max(summary_scores, axis=-1)))
        window_weights = jnp.exp(window_scores - peak[..., None])
        summary_weights = jnp.exp(summary_scores - peak[..., None])
        denominator = lax.optimization_barrier(jnp.sum(window_weights, axis=-1)) + lax.optimization_barrier(jnp.sum(summary_weights, axis=-1))
        rounded_window = lax.optimization_barrier(window_weights.astype(jnp.bfloat16)).astype(jnp.float32)
        rounded_summary = lax.optimization_barrier(summary_weights.astype(jnp.bfloat16)).astype(jnp.float32)
        numerator = jnp.einsum('hqk,khd->hqd', rounded_window, window_values)
        numerator = numerator + jnp.einsum('hqj,jhd->hqd', rounded_summary, summary_values)
        result = numerator / denominator[..., None]
        return jnp.transpose(result, (1, 0, 2)).reshape(BLOCK, HEADS * HEAD_DIM).astype(jnp.bfloat16)
    outputs = lax.map(one_block, block_ids)
    return outputs.reshape(SEQ, HEADS * HEAD_DIM)
```

```python
import functools
import itertools
import math

import jax
import jax.numpy as jnp
import numpy as np
from jax import lax
from jax.experimental import pallas as pl
from jax.experimental.pallas import tpu as pltpu
from jax.sharding import PartitionSpec as P

HEADS = 32
HEAD_DIM = 128
BLOCK = 128
AXES = ("grp", "seq")
NZ, NY, NCORE, NX = 8, 4, 2, 4
HALF = HEADS * HEAD_DIM // 2
HB = 4
COLS = HB * HEAD_DIM
STEPS = HALF // COLS
LOG2E = 1.4426950408889634


def device_index(z, y, core, x):
    return (((z * 2 + y // 2) * 2 + core) * 2 + y % 2) * 4 + x


def receive(value, axis, by):
    pairs = []
    for z, y, core, x in itertools.product(range(NZ), range(NY), range(NCORE), range(NX)):
        step = by[core] if isinstance(by, tuple) else by
        to = [z, y, core, x]
        at = "zycx".index(axis)
        to[at] = (to[at] - step) % (NZ, NY, NCORE, NX)[at]
        pairs.append((device_index(z, y, core, x), device_index(*to)))
    return lax.ppermute(value, AXES, pairs)


def shifted(value, by):
    count = lax.axis_size(AXES)
    pairs = [(i, i + by) for i in range(count) if 0 <= i + by < count]
    return lax.ppermute(value, AXES, pairs)


def pool_kernel(k_ref, v_ref, s_ref, last0_ref, first0_ref, last1_ref, first1_ref):
    step = pl.program_id(0)
    for which, ref in enumerate((k_ref, v_ref)):
        for block in range(2):
            mean = jnp.sum(
                ref[block * BLOCK : (block + 1) * BLOCK, :].astype(jnp.float32), axis=0, keepdims=True
            ) * (1.0 / BLOCK)
            for h in range(HB):
                one = mean[:, h * HEAD_DIM : (h + 1) * HEAD_DIM]
                spread = jnp.mean(one * one, axis=-1, keepdims=True)
                s_ref[which, block : block + 1, h * HEAD_DIM : (h + 1) * HEAD_DIM] = (
                    one / jnp.sqrt(spread + 1e-06)
                )

    @pl.when(step < STEPS)
    def _():
        for which, ref in enumerate((k_ref, v_ref)):
            first0_ref[which] = ref[:BLOCK, :]
            last0_ref[which] = ref[BLOCK:, :]

    @pl.when(step >= STEPS)
    def _():
        for which, ref in enumerate((k_ref, v_ref)):
            first1_ref[which] = ref[:BLOCK, :]
            last1_ref[which] = ref[BLOCK:, :]


def pool(keys, values):
    rows, width = keys.shape
    block = pl.BlockSpec((rows, COLS), lambda c: (0, c))
    edge0 = pl.BlockSpec((2, BLOCK, COLS), lambda c: (0, 0, jnp.minimum(c, STEPS - 1)))
    edge1 = pl.BlockSpec((2, BLOCK, COLS), lambda c: (0, 0, jnp.maximum(c - STEPS, 0)))
    edge_shape = jax.ShapeDtypeStruct((2, BLOCK, HALF), keys.dtype)
    return pl.pallas_call(
        pool_kernel,
        grid=(width // COLS,),
        in_specs=[block, block],
        out_specs=[pl.BlockSpec((2, 2, COLS), lambda c: (0, 0, c)), edge0, edge0, edge1, edge1],
        out_shape=[jax.ShapeDtypeStruct((2, 2, width), jnp.float32)] + [edge_shape] * 4,
        cost_estimate=pl.CostEstimate(flops=4_000_000_000, bytes_accessed=8 << 20, transcendentals=0),
        name="pool",
    )(keys, values)


def attend_kernel(n_pieces, edge_ref, gpos_ref, bias_ref, q_ref, k_ref, v_ref, left_ref, right_ref, *rest):
    sk_refs, sv_refs = rest[:n_pieces], rest[n_pieces : 2 * n_pieces]
    out_ref, full_bias = rest[-2], rest[-1]
    rows = q_ref.shape[0]
    items = bias_ref.shape[1]

    @pl.when(pl.program_id(0) == 0)
    def _():
        for block in range(2):
            row = lax.broadcasted_iota(jnp.int32, (BLOCK, items), 0)
            listed = jnp.broadcast_to(bias_ref[block : block + 1, :], (BLOCK, items))
            full_bias[block * BLOCK : (block + 1) * BLOCK, BLOCK:] = jnp.where(
                row == gpos_ref[block], 0.0, listed
            )
            full_bias[block * BLOCK : (block + 1) * BLOCK, :BLOCK] = jnp.where(
                edge_ref[block] > 0, jnp.zeros((BLOCK, BLOCK), jnp.float32), -jnp.inf
            )

    scale = LOG2E / math.sqrt(HEAD_DIM)
    nt = (((1,), (1,)), ((), ()))
    ones = jnp.ones((rows + items, HEAD_DIM), jnp.bfloat16)
    for h in range(HB):
        at = slice(h * HEAD_DIM, (h + 1) * HEAD_DIM)
        q = q_ref[:, at]
        ks = jnp.concatenate([k_ref[:, at]] + [r[:, at] for r in sk_refs], axis=0)
        vs = jnp.concatenate([v_ref[:, at]] + [r[:, at] for r in sv_refs], axis=0)
        s_main = lax.dot_general(q, ks, nt, preferred_element_type=jnp.float32) * scale
        s_edge = jnp.concatenate(
            [
                lax.dot_general(q[:BLOCK], left_ref[0, :, at], nt, preferred_element_type=jnp.float32),
                lax.dot_general(q[BLOCK:], right_ref[0, :, at], nt, preferred_element_type=jnp.float32),
            ],
            axis=0,
        ) * scale + full_bias[:, :BLOCK]
        s_window = s_main[:, :rows]
        s_sum = s_main[:, rows:] + full_bias[:, BLOCK:]
        peak = jnp.maximum(
            jnp.maximum(jnp.max(s_window, axis=1, keepdims=True), jnp.max(s_sum, axis=1, keepdims=True)),
            jnp.max(s_edge, axis=1, keepdims=True),
        )
        w_main = jnp.concatenate(
            [jnp.exp2(s_window - peak).astype(jnp.bfloat16), jnp.exp2(s_sum - peak).astype(jnp.bfloat16)], axis=1
        )
        w_edge = jnp.exp2(s_edge - peak).astype(jnp.bfloat16)
        total = jnp.dot(
            w_main, jnp.concatenate([vs, ones], axis=1), preferred_element_type=jnp.float32
        )
        for block, ref in enumerate((left_ref, right_ref)):
            part = slice(block * BLOCK, (block + 1) * BLOCK)
            both = total[part] + jnp.dot(
                w_edge[part],
                jnp.concatenate([ref[1, :, at], ones[:BLOCK]], axis=1),
                preferred_element_type=jnp.float32,
            )
            out_ref[part, at] = (both[:, :HEAD_DIM] / both[:, HEAD_DIM:]).astype(out_ref.dtype)


def attend(half, edge_ok, gpos, bias, queries, keys, values, left, right, pieces, out):
    rows, width = queries.shape
    wide = pl.BlockSpec((rows, COLS), lambda c: (0, half * STEPS + c))
    edge = pl.BlockSpec((2, BLOCK, COLS), lambda c: (0, 0, c))
    smem = pl.BlockSpec(memory_space=pltpu.SMEM)
    n = len(pieces)
    in_specs = [smem, smem, pl.BlockSpec(bias.shape, lambda c: (0, 0)), wide, wide, wide, edge, edge]
    in_specs += [pl.BlockSpec((p.shape[0], COLS), lambda c: (0, c)) for p in pieces]
    in_specs += [pl.BlockSpec((p.shape[0], COLS), lambda c: (0, STEPS + c)) for p in pieces]
    args = [edge_ok, gpos, bias, queries, keys, values, left, right, *pieces, *pieces]
    aliases = {}
    if out is not None:
        in_specs.append(pl.BlockSpec(memory_space=pl.ANY))
        aliases = {len(args): 0}
        args.append(out)
    return pl.pallas_call(
        functools.partial(attend_kernel, n),
        grid=(STEPS,),
        in_specs=in_specs,
        out_specs=wide,
        out_shape=jax.ShapeDtypeStruct((rows, width), queries.dtype),
        scratch_shapes=[pltpu.VMEM((rows, BLOCK + bias.shape[1]), jnp.float32)],
        input_output_aliases=aliases,
        cost_estimate=pl.CostEstimate(flops=4_000_000_000, bytes_accessed=8 << 20, transcendentals=0),
        name="attend",
    )(*args)


def gather_same_core(value):
    pieces = [value] + [receive(value, "x", j) for j in (1, 3, 2)]
    value = jnp.concatenate(pieces, axis=0)
    return value


X_ORDER = (0, 1, 3, 2)
Z_ORDER = (0, 4, 2, 6, 1, 5, 3, 7)
Y_ORDER = (0, 1, 3, 2)


def gather_z(value):
    for step in (4, 2, 1):
        value = jnp.concatenate([value, receive(value, "z", (step, -step))], axis=0)
    return value


def gathered_ids(position):
    x, rest = position % NX, position // NX
    y_lo, rest = rest % 2, rest // 2
    core, rest = rest % 2, rest // 2
    y, z = (rest % 2) * 2 + y_lo, rest // 2
    offsets = np.array(list(itertools.product((0, 1), Y_ORDER, Z_ORDER, X_ORDER, (0, 1))), np.int32)
    swap, dy, dz, dx, row = (jnp.asarray(offsets[:, i]) for i in range(5))
    whose = jnp.where(swap == 1, 1 - core, core)
    z_at = (z + jnp.where(whose == 0, dz, -dz) + NZ) % NZ
    return 2 * device_index(z_at, (y + dy) % NY, whose, (x + dx) % NX) + row


def shards(queries, keys, values, global_pos, layout):
    position = lax.axis_index(AXES)
    devices = lax.axis_size(AXES)
    sums, last0, first0, last1, first1 = pool(keys, values)
    sums = sums.astype(jnp.bfloat16).reshape(2, 2, 2, HALF)
    sums = jnp.transpose(sums, (1, 2, 0, 3)).reshape(2, 4 * HALF)
    lined = gather_same_core(sums)
    last0, first0, last1, first1, lined = lax.optimization_barrier((last0, first0, last1, first1, lined))
    left0, right0 = shifted(last0, 1), shifted(first0, -1)
    left1, right1 = shifted(last1, 1), shifted(first1, -1)
    ids = gathered_ids(position)
    listed = jnp.any(layout[:, :, None] == ids[None, None, :], axis=1)
    bias = jnp.where(listed, 0.0, -jnp.inf).astype(jnp.float32)
    edge_ok = jnp.stack([position > 0, position < devices - 1]).astype(jnp.int32)
    out = None
    for half in range(2):
        part = gather_z(lined[:, half * 2 * HALF : (half + 1) * 2 * HALF])
        pieces = [part] + [receive(part, "y", j) for j in (1, 3, 2)]
        pieces = pieces + [receive(p, "c", 1) for p in pieces]
        out = attend(
            half, edge_ok, global_pos, bias, queries, keys, values,
            *((left0, right0) if half == 0 else (left1, right1)), pieces, out,
        )
    return out


def solution(mesh):
    in_specs = (
        P(("grp", "seq"), None),
        P(("grp", "seq"), None),
        P(("grp", "seq"), None),
        P(("grp", "seq")),
        P(("grp", "seq"), None),
    )
    out_specs = P(("grp", "seq"), None)
    return jax.shard_map(shards, mesh=mesh, in_specs=in_specs, out_specs=out_specs, check_vma=False)
```

```python
import functools
import itertools
import math

import jax
import jax.numpy as jnp
import numpy as np
from jax import lax
from jax.experimental import pallas as pl
from jax.experimental.pallas import tpu as pltpu
from jax.sharding import PartitionSpec as P


HEAD_DIM = 128
BLOCK = 128
AXES = ("grp", "seq")
NZ, NY, NCORE, NX = 8, 4, 2, 4
HB = 4
COLS = HB * HEAD_DIM
LOG2E = 1.4426950408889634


def device_index(z, y, core, x):
    return (((z * 2 + y // 2) * 2 + core) * 2 + y % 2) * 4 + x


def receive(value, axis, by):
    pairs = []
    for z, y, core, x in itertools.product(range(NZ), range(NY), range(NCORE), range(NX)):
        to = [z, y, core, x]
        at = "zycx".index(axis)
        step = by(y, core, x) if callable(by) else by
        to[at] = (to[at] - step) % (NZ, NY, NCORE, NX)[at]
        pairs.append((device_index(z, y, core, x), device_index(*to)))
    return lax.ppermute(value, AXES, pairs)


def long_way(y, core, x):
    crosses = (y, x) in ((0, 0), (NY - 1, NX - 1))
    return (1 - 2 * core) * (-1 if crosses else 1)


PLANE = NX * NY * NCORE


def shifted(value, by):
    count = lax.axis_size(AXES)
    pairs = [(i, i + by) for i in range(count) if 0 <= i + by < count]
    return lax.ppermute(value, AXES, [(i, j) for i, j in pairs if i // PLANE == j // PLANE])


def crossed(value, by, hop):
    count = lax.axis_size(AXES)
    pairs = [(i, i + by * PLANE, i + by) for i in range(count) if 0 <= i + by < count]
    return lax.ppermute(value, AXES, [places[hop : hop + 2] for places in pairs if places[0] // PLANE != places[2] // PLANE])


def pool_kernel(k_hbm, v_hbm, s_ref, last, first, buf, in_sems, out_sems):
    chunks = buf.shape[2] // COLS

    def load(which, c):
        at = pl.ds(c * COLS, COLS)
        source = (k_hbm, v_hbm)[which]
        return pltpu.make_async_copy(source.at[:, at], buf.at[which, :, at], in_sems.at[which, c])

    def save(which, c, end):
        at = pl.ds(c * COLS, COLS)
        return pltpu.make_async_copy(
            buf.at[which, pl.ds(end * BLOCK, BLOCK), at], (first, last)[end].at[which, :, at], out_sems.at[which, end, c]
        )

    for c in range(chunks):
        for which in range(2):
            load(which, c).start()
    for c in range(chunks):
        for which in range(2):
            load(which, c).wait()
            for end in range(2):
                save(which, c, end).start()
            for h in range(HB):
                at = c * COLS + h * HEAD_DIM
                rows = []
                for block in range(2):
                    tokens = buf[which, block * BLOCK : (block + 1) * BLOCK, at : at + HEAD_DIM]
                    one = jnp.sum(tokens.astype(jnp.float32), axis=0, keepdims=True) * (1.0 / BLOCK)
                    spread = jnp.mean(one * one, axis=-1, keepdims=True)
                    rows.append(one / jnp.sqrt(spread + 1e-06))
                to = which * buf.shape[2] + at
                s_ref[:, to : to + HEAD_DIM] = jnp.concatenate(rows, axis=0).astype(s_ref.dtype)
    for c in range(chunks):
        for which in range(2):
            for end in range(2):
                save(which, c, end).wait()


def pool(keys, values):
    rows, width = keys.shape
    chunks = width // COLS
    hbm = pl.BlockSpec(memory_space=pl.ANY)
    edge_shape = jax.ShapeDtypeStruct((2, BLOCK, width), keys.dtype)
    return pl.pallas_call(
        pool_kernel,
        in_specs=[hbm, hbm],
        out_specs=[pl.BlockSpec(memory_space=pltpu.VMEM)] + [hbm] * 2,
        out_shape=[jax.ShapeDtypeStruct((2, 2 * width), keys.dtype)] + [edge_shape] * 2,
        scratch_shapes=[
            pltpu.VMEM((2, rows, width), keys.dtype),
            pltpu.SemaphoreType.DMA((2, chunks)),
            pltpu.SemaphoreType.DMA((2, 2, chunks)),
        ],
        cost_estimate=pl.CostEstimate(flops=4_000_000_000, bytes_accessed=8 << 20, transcendentals=0),
        name="pool",
    )(keys, values)


def attend_kernel(n_pieces, at_ref, listed_ref, q_ref, k_ref, v_ref, *rest):
    left_refs, right_refs, rest = rest[:2], rest[2:4], rest[4:]
    sk_refs, sv_refs = rest[:n_pieces], rest[n_pieces : 2 * n_pieces]
    out_ref, bias_ref = rest[-2], rest[-1]
    rows = q_ref.shape[0]
    items = listed_ref.shape[1]
    parts = [slice(b * BLOCK, (b + 1) * BLOCK) for b in range(2)]

    @pl.when(pl.program_id(0) == 0)
    def _():
        for b in range(2):
            row = lax.broadcasted_iota(jnp.int32, (BLOCK, items), 0)
            listed = jnp.broadcast_to(listed_ref[b : b + 1, :], (BLOCK, items))
            bias_ref[parts[b], BLOCK:] = jnp.where(row == at_ref[2 + b], 0.0, listed)
            bias_ref[parts[b], :BLOCK] = jnp.where(at_ref[b] > 0, jnp.zeros((BLOCK, BLOCK), jnp.float32), -jnp.inf)

    scale = LOG2E / math.sqrt(HEAD_DIM)
    nt = (((1,), (1,)), ((), ()))

    def dot(x, y, dims=(((1,), (0,)), ((), ()))):
        return lax.dot_general(x, y, dims, preferred_element_type=jnp.float32)

    edges = [
        [jnp.where(at_ref[4 + side] == 0, refs[0][kv], refs[1][kv]) for kv in range(2)]
        for side, refs in enumerate((left_refs, right_refs))
    ]
    ones = jnp.ones((rows + items, HEAD_DIM), jnp.bfloat16)
    for h in range(HB):
        at = slice(h * HEAD_DIM, (h + 1) * HEAD_DIM)
        q = q_ref[:, at]
        ks = jnp.concatenate([k_ref[:, at]] + [r[:, at] for r in sk_refs], axis=0)
        vs = jnp.concatenate([v_ref[:, at]] + [r[:, at] for r in sv_refs], axis=0)
        s_main = dot(q, ks, nt) * scale
        s_edge = jnp.concatenate([dot(q[parts[b]], edges[b][0][:, at], nt) for b in range(2)], axis=0)
        s_edge = s_edge * scale + bias_ref[:, :BLOCK]
        s_window = s_main[:, :rows]
        s_sum = s_main[:, rows:] + bias_ref[:, BLOCK:]
        peak = jnp.maximum(
            jnp.maximum(jnp.max(s_window, axis=1, keepdims=True), jnp.max(s_sum, axis=1, keepdims=True)),
            jnp.max(s_edge, axis=1, keepdims=True),
        )
        w_main = jnp.concatenate(
            [jnp.exp2(s_window - peak).astype(jnp.bfloat16), jnp.exp2(s_sum - peak).astype(jnp.bfloat16)], axis=1
        )
        w_edge = jnp.exp2(s_edge - peak).astype(jnp.bfloat16)
        total = dot(w_main, jnp.concatenate([vs, ones], axis=1))
        for b in range(2):
            both = total[parts[b]] + dot(
                w_edge[parts[b]], jnp.concatenate([edges[b][1][:, at], ones[:BLOCK]], axis=1)
            )
            out_ref[parts[b], at] = (both[:, :HEAD_DIM] / both[:, HEAD_DIM:]).astype(out_ref.dtype)


def attend(at, listed, queries, keys, values, lefts, rights, pieces):
    rows, width = queries.shape
    steps = width // COLS
    wide = pl.BlockSpec((rows, COLS), lambda c, at: (0, c))


    def edge(side, which):
        return pl.BlockSpec((2, BLOCK, COLS), lambda c, at: (0, 0, jnp.where(at[4 + side] == which, c, 0)))

    in_specs = [pl.BlockSpec(listed.shape, lambda c, at: (0, 0)), wide, wide, wide]
    in_specs += [edge(side, which) for side in range(2) for which in range(2)]
    in_specs += [pl.BlockSpec((p.shape[0], COLS), lambda c, at: (0, c)) for p in pieces]
    in_specs += [pl.BlockSpec((p.shape[0], COLS), lambda c, at: (0, steps + c)) for p in pieces]
    return pl.pallas_call(
        functools.partial(attend_kernel, len(pieces)),
        grid_spec=pltpu.PrefetchScalarGridSpec(
            num_scalar_prefetch=1,
            grid=(steps,),
            in_specs=in_specs,
            out_specs=wide,
            scratch_shapes=[pltpu.VMEM((rows, BLOCK + listed.shape[1]), jnp.float32)],
        ),
        out_shape=jax.ShapeDtypeStruct((rows, width), queries.dtype),
        cost_estimate=pl.CostEstimate(flops=8_000_000_000, bytes_accessed=16 << 20, transcendentals=0),
        name="attend",
    )(at, listed, queries, keys, values, *lefts, *rights, *pieces, *pieces)


X_ORDER = (0, 1, 3, 2)
Y_ORDER = (0, 1, 3, 2)


def gathered_ids(position):
    x, rest = position % NX, position // NX
    y_lo, rest = rest % 2, rest // 2
    core, rest = rest % 2, rest // 2
    y, z = (rest % 2) * 2 + y_lo, rest // 2
    offsets = np.array(
        list(itertools.product((0, 1), (0, 1, 2, 3, 4, -1, -2, -3), Y_ORDER, X_ORDER, (0, 1))), np.int32
    )
    swap, dz, dy, dx, row = (jnp.asarray(offsets[:, i]) for i in range(5))
    whose = jnp.where(swap == 1, 1 - core, core)
    crosses = ((y == 0) & (x == 0)) | ((y == NY - 1) & (x == NX - 1))
    way = (1 - 2 * whose) * jnp.where(crosses, -1, 1)
    return 2 * device_index((z + way * dz + NZ) % NZ, (y + dy) % NY, whose, (x + dx) % NX) + row


def work(queries, keys, values, global_pos, layout):
    position = lax.axis_index(AXES)
    devices = lax.axis_size(AXES)
    lined, last, first = pool(keys, values)
    for axis, order in (("x", X_ORDER), ("y", Y_ORDER)):
        pieces = [lined]
        for j in order[1:]:
            pieces.append(receive(lined, axis, j))
        lined = jnp.concatenate(pieces, axis=0)
    edges = []
    for source, by in ((last, 1), (first, -1)):
        inside = shifted(source, by)
        between = crossed(source, by, 0)
        edges.append([inside, crossed(between, by, 1)])
    lefts, rights = edges
    ids = gathered_ids(position)
    listed = jnp.any(layout[:, :, None] == ids[None, None, :], axis=1)
    listed = jnp.where(listed, 0.0, -jnp.inf).astype(jnp.float32)
    at = jnp.stack(
        [position > 0, position < devices - 1, position % PLANE == 0, position % PLANE == PLANE - 1]
    ).astype(jnp.int32)
    at = jnp.concatenate([at[:2], global_pos, at[2:]])
    mine = [lined]
    for name, steps, sign in (("long", 4, 1), ("short", 3, -1)):
        passed = lined
        for step in range(steps):
            passed = receive(passed, "z", lambda *place: sign * long_way(*place))
            if (name, step) == ("long", 0):
                passed, listed, at = lax.optimization_barrier((passed, listed, at))
            mine.append(passed)
    other = []
    for p in mine:
        other.append(receive(p, "c", 1))
    return attend(at, listed, queries, keys, values, lefts, rights, mine + other)


def solution(mesh):
    in_specs = (
        P(("grp", "seq"), None),
        P(("grp", "seq"), None),
        P(("grp", "seq"), None),
        P(("grp", "seq")),
        P(("grp", "seq"), None),
    )
    out_specs = P(("grp", "seq"), None)
    return jax.shard_map(work, mesh=mesh, in_specs=in_specs, out_specs=out_specs, check_vma=False)
```

```python
import functools
import itertools
import math

import jax
import jax.numpy as jnp
import numpy as np
from jax import lax
from jax.experimental import pallas as pl
from jax.experimental.pallas import tpu as pltpu
from jax.sharding import PartitionSpec as P


HEAD_DIM = 128
BLOCK = 128
AXES = ("grp", "seq")
NZ, NY, NCORE, NX = 8, 4, 2, 4
HB = 8
COLS = HB * HEAD_DIM
GROUP = 4
LOG2E = 1.4426950408889634


def device_index(z, y, core, x):
    return (((z * 2 + y // 2) * 2 + core) * 2 + y % 2) * 4 + x


def receive(value, axis, by):
    pairs = []
    for z, y, core, x in itertools.product(range(NZ), range(NY), range(NCORE), range(NX)):
        to = [z, y, core, x]
        at = "zycx".index(axis)
        step = by(y, core, x) if callable(by) else by
        to[at] = (to[at] - step) % (NZ, NY, NCORE, NX)[at]
        pairs.append((device_index(z, y, core, x), device_index(*to)))
    return lax.ppermute(value, AXES, pairs)


def long_way(y, core, x):
    crosses = (y, x) in ((0, 0), (NY - 1, NX - 1))
    return (1 - 2 * core) * (-1 if crosses else 1)


PLANE = NX * NY * NCORE


def shifted(value, by):
    count = lax.axis_size(AXES)
    pairs = [(i, i + by) for i in range(count) if 0 <= i + by < count]
    return lax.ppermute(value, AXES, [(i, j) for i, j in pairs if i // PLANE == j // PLANE])


def crossed(value, by, hop):
    count = lax.axis_size(AXES)
    pairs = [(i, i + by * PLANE, i + by) for i in range(count) if 0 <= i + by < count]
    return lax.ppermute(value, AXES, [places[hop : hop + 2] for places in pairs if places[0] // PLANE != places[2] // PLANE])


def pool_kernel(k_hbm, v_hbm, s_ref, last, first, buf, in_sems, out_sems):
    chunks = buf.shape[2] // COLS

    def load(which, c):
        at = pl.ds(c * COLS, COLS)
        source = (k_hbm, v_hbm)[which]
        return pltpu.make_async_copy(source.at[:, at], buf.at[which, :, at], in_sems.at[which, c])

    def save(which, c, end):
        at = pl.ds(c * COLS, COLS)
        return pltpu.make_async_copy(
            buf.at[which, pl.ds(end * BLOCK, BLOCK), at], (first, last)[end].at[which, :, at], out_sems.at[which, end, c]
        )

    for c in range(chunks):
        for which in range(2):
            load(which, c).start()
    for c in range(chunks):
        for which in range(2):
            load(which, c).wait()
            for end in range(2):
                save(which, c, end).start()
            for h in range(HB):
                at = c * COLS + h * HEAD_DIM
                rows = []
                for block in range(2):
                    tokens = buf[which, block * BLOCK : (block + 1) * BLOCK, at : at + HEAD_DIM]
                    one = jnp.sum(tokens.astype(jnp.float32), axis=0, keepdims=True) * (1.0 / BLOCK)
                    spread = jnp.mean(one * one, axis=-1, keepdims=True)
                    rows.append(one / jnp.sqrt(spread + 1e-06))
                to = which * buf.shape[2] + at
                s_ref[:, to : to + HEAD_DIM] = jnp.concatenate(rows, axis=0).astype(s_ref.dtype)
    for c in range(chunks):
        for which in range(2):
            for end in range(2):
                save(which, c, end).wait()


def pool(keys, values):
    rows, width = keys.shape
    chunks = width // COLS
    hbm = pl.BlockSpec(memory_space=pl.ANY)
    edge_shape = jax.ShapeDtypeStruct((2, BLOCK, width), keys.dtype)
    return pl.pallas_call(
        pool_kernel,
        in_specs=[hbm, hbm],
        out_specs=[pl.BlockSpec(memory_space=pltpu.VMEM)] + [hbm] * 2,
        out_shape=[jax.ShapeDtypeStruct((2, 2 * width), keys.dtype)] + [edge_shape] * 2,
        scratch_shapes=[
            pltpu.VMEM((2, rows, width), keys.dtype),
            pltpu.SemaphoreType.DMA((2, chunks)),
            pltpu.SemaphoreType.DMA((2, 2, chunks)),
        ],
        cost_estimate=pl.CostEstimate(flops=4_000_000_000, bytes_accessed=8 << 20, transcendentals=0),
        name="pool",
    )(keys, values)


SCALE = LOG2E / math.sqrt(HEAD_DIM)
HEAD_AT = [slice(h * HEAD_DIM, (h + 1) * HEAD_DIM) for h in range(HB)]
BLOCK_AT = [slice(b * BLOCK, (b + 1) * BLOCK) for b in range(2)]


def dot(x, y):
    return jnp.dot(x, y, preferred_element_type=jnp.float32)


def score(q, k):
    return lax.dot_general(q, k, (((1,), (1,)), ((), ())), preferred_element_type=jnp.float32) * SCALE


def own_kernel(q_ref, k_ref, v_ref, out_ref, level_ref):
    rows = q_ref.shape[0]
    ones = jnp.ones((rows, HEAD_DIM), jnp.bfloat16)
    lane = lax.broadcasted_iota(jnp.int32, (rows, HEAD_DIM), 1)
    scores = [score(q_ref[:, at], k_ref[:, at]) for at in HEAD_AT]
    peaks = [jnp.max(s, axis=1, keepdims=True) for s in scores]
    weights = [jnp.exp2(s - peak).astype(jnp.bfloat16) for s, peak in zip(scores, peaks)]
    level = jnp.zeros((rows, HEAD_DIM), jnp.float32)
    for h, at in enumerate(HEAD_AT):
        both = dot(weights[h], jnp.concatenate([v_ref[:, at], ones], axis=1))
        total = both[:, HEAD_DIM:]
        out_ref[:, at] = (both[:, :HEAD_DIM] / total).astype(out_ref.dtype)
        level = jnp.where(lane == h, peaks[h] + jnp.log(total) * LOG2E, level)
    level_ref[0] = level


def own(queries, keys, values):
    rows, width = queries.shape
    steps = width // COLS
    wide = pl.BlockSpec((rows, COLS), lambda c: (0, c))
    return pl.pallas_call(
        own_kernel,
        grid=(steps,),
        in_specs=[wide, wide, wide],
        out_specs=[wide, pl.BlockSpec((1, rows, HEAD_DIM), lambda c: (c, 0, 0))],
        out_shape=[
            jax.ShapeDtypeStruct((rows, width), jnp.float32),
            jax.ShapeDtypeStruct((steps, rows, HEAD_DIM), jnp.float32),
        ],
        cost_estimate=pl.CostEstimate(flops=2_000_000_000, bytes_accessed=9 << 20, transcendentals=0),
        compiler_params=pltpu.CompilerParams(vmem_limit_bytes=24 << 20),
        name="own",
    )(queries, keys, values)


def attend_kernel(n_pieces, at_ref, listed_ref, q_ref, own_ref, level_ref, *rest):
    left_refs, right_refs, rest = rest[:2], rest[2:4], rest[4:]
    sk_refs, sv_refs = rest[:n_pieces], rest[n_pieces : 2 * n_pieces]
    out_ref, bias_ref, edge_ref = rest[-3:]
    items = listed_ref.shape[1]

    @pl.when(pl.program_id(0) == 0)
    def _():
        for b in range(2):
            row = lax.broadcasted_iota(jnp.int32, (BLOCK, items), 0)
            listed = jnp.broadcast_to(listed_ref[b : b + 1, :], (BLOCK, items))
            bias_ref[BLOCK_AT[b], BLOCK:] = jnp.where(row == at_ref[2 + b], 0.0, listed)
            bias_ref[BLOCK_AT[b], :BLOCK] = jnp.where(at_ref[b] > 0, jnp.zeros((BLOCK, BLOCK), jnp.float32), -jnp.inf)

    for side, refs in enumerate((left_refs, right_refs)):
        for which in range(2):

            @pl.when(at_ref[4 + side] == which)
            def _(side=side, ref=refs[which]):
                edge_ref[side] = ref[...]

    ones = jnp.ones((items, HEAD_DIM), jnp.bfloat16)
    levels = [jnp.broadcast_to(level_ref[0, :, h : h + 1], (2 * BLOCK, HEAD_DIM)) for h in range(HB)]
    for group in range(0, HB, GROUP):
        heads = range(group, group + GROUP)
        sums, edges = {}, {}
        for h in heads:
            at = HEAD_AT[h]
            ks = jnp.concatenate([r[:, at] for r in sk_refs], axis=0)
            sums[h] = score(q_ref[:, at], ks) + bias_ref[:, BLOCK:]
            edges[h] = [
                score(q_ref[BLOCK_AT[b], at], edge_ref[b, 0, :, at]) + bias_ref[BLOCK_AT[b], :BLOCK] for b in range(2)
            ]
        w_sum, w_edge, w_own = {}, {}, {}
        for h in heads:
            top = jnp.maximum(jnp.concatenate(edges[h], axis=0), levels[h])
            for c in range(0, items, BLOCK):
                top = jnp.maximum(top, sums[h][:, c : c + BLOCK])
            peak = jnp.max(top, axis=1, keepdims=True)
            w_sum[h] = jnp.exp2(sums[h] - peak).astype(jnp.bfloat16)
            w_edge[h] = [jnp.exp2(edges[h][b] - peak[BLOCK_AT[b]]).astype(jnp.bfloat16) for b in range(2)]
            w_own[h] = jnp.exp2(levels[h] - peak)
        for h in heads:
            at = HEAD_AT[h]
            vs = jnp.concatenate([r[:, at] for r in sv_refs], axis=0)
            total = dot(w_sum[h], jnp.concatenate([vs, ones], axis=1))
            for b in range(2):
                both = total[BLOCK_AT[b]] + dot(
                    w_edge[h][b], jnp.concatenate([edge_ref[b, 1, :, at], ones[:BLOCK]], axis=1)
                )
                mine = w_own[h][BLOCK_AT[b]]
                up = both[:, :HEAD_DIM] + mine * own_ref[BLOCK_AT[b], at]
                out_ref[BLOCK_AT[b], at] = (up / (both[:, HEAD_DIM:] + mine)).astype(out_ref.dtype)


def attend(at, listed, queries, seen, level, lefts, rights, pieces):
    rows, width = queries.shape
    steps = width // COLS
    wide = pl.BlockSpec((rows, COLS), lambda c, at: (0, c))


    def edge(side, which):
        return pl.BlockSpec((2, BLOCK, COLS), lambda c, at: (0, 0, jnp.where(at[4 + side] == which, c, 0)))

    in_specs = [pl.BlockSpec(listed.shape, lambda c, at: (0, 0)), wide, wide]
    in_specs += [pl.BlockSpec((1, rows, HEAD_DIM), lambda c, at: (c, 0, 0))]
    in_specs += [edge(side, which) for side in range(2) for which in range(2)]
    in_specs += [pl.BlockSpec((p.shape[0], COLS), lambda c, at: (0, c)) for p in pieces]
    in_specs += [pl.BlockSpec((p.shape[0], COLS), lambda c, at: (0, steps + c)) for p in pieces]
    return pl.pallas_call(
        functools.partial(attend_kernel, len(pieces)),
        grid_spec=pltpu.PrefetchScalarGridSpec(
            num_scalar_prefetch=1,
            grid=(steps,),
            in_specs=in_specs,
            out_specs=wide,
            scratch_shapes=[
                pltpu.VMEM((rows, BLOCK + listed.shape[1]), jnp.float32),
                pltpu.VMEM((2, 2, BLOCK, COLS), queries.dtype),
            ],
        ),
        out_shape=jax.ShapeDtypeStruct((rows, width), queries.dtype),
        cost_estimate=pl.CostEstimate(flops=8_000_000_000, bytes_accessed=16 << 20, transcendentals=0),
        compiler_params=pltpu.CompilerParams(vmem_limit_bytes=26 << 20),
        name="attend",
    )(at, listed, queries, seen, level, *lefts, *rights, *pieces, *pieces)


X_ORDER = (0, 1, 3, 2)
Y_ORDER = (0, 1, 3, 2)


def gathered_ids(position):
    x, rest = position % NX, position // NX
    y_lo, rest = rest % 2, rest // 2
    core, rest = rest % 2, rest // 2
    y, z = (rest % 2) * 2 + y_lo, rest // 2
    offsets = np.array(
        list(itertools.product((0, 1), (0, 1, 2, 3, 4, -1, -2, -3), Y_ORDER, X_ORDER, (0, 1))), np.int32
    )
    swap, dz, dy, dx, row = (jnp.asarray(offsets[:, i]) for i in range(5))
    whose = jnp.where(swap == 1, 1 - core, core)
    crosses = ((y == 0) & (x == 0)) | ((y == NY - 1) & (x == NX - 1))
    way = (1 - 2 * whose) * jnp.where(crosses, -1, 1)
    return 2 * device_index((z + way * dz + NZ) % NZ, (y + dy) % NY, whose, (x + dx) % NX) + row


def work(queries, keys, values, global_pos, layout):
    position = lax.axis_index(AXES)
    devices = lax.axis_size(AXES)
    lined, last, first = pool(keys, values)
    for axis, order in (("x", X_ORDER), ("y", Y_ORDER)):
        pieces = [lined]
        for j in order[1:]:
            pieces.append(receive(lined, axis, j))
        lined = jnp.concatenate(pieces, axis=0)
    edges = []
    for source, by in ((last, 1), (first, -1)):
        inside = shifted(source, by)
        between = crossed(source, by, 0)
        edges.append([inside, crossed(between, by, 1)])
    lefts, rights = edges
    ids = gathered_ids(position)
    listed = jnp.any(layout[:, :, None] == ids[None, None, :], axis=1)
    listed = jnp.where(listed, 0.0, -jnp.inf).astype(jnp.float32)
    at = jnp.stack(
        [position > 0, position < devices - 1, position % PLANE == 0, position % PLANE == PLANE - 1]
    ).astype(jnp.int32)
    at = jnp.concatenate([at[:2], global_pos, at[2:]])
    own_in = lax.optimization_barrier((queries, keys, values, lined))
    seen, level = own(*own_in[:3])
    mine = [lined]
    for name, steps, sign in (("long", 4, 1), ("short", 3, -1)):
        passed = lined
        for step in range(steps):
            passed = receive(passed, "z", lambda *place: sign * long_way(*place))
            if (name, step) == ("long", 0):
                passed, listed, at = lax.optimization_barrier((passed, listed, at))
            mine.append(passed)
    other = []
    for p in mine:
        other.append(receive(p, "c", 1))
    return attend(at, listed, queries, seen, level, lefts, rights, mine + other)


def solution(mesh):
    in_specs = (
        P(("grp", "seq"), None),
        P(("grp", "seq"), None),
        P(("grp", "seq"), None),
        P(("grp", "seq")),
        P(("grp", "seq"), None),
    )
    out_specs = P(("grp", "seq"), None)
    return jax.shard_map(work, mesh=mesh, in_specs=in_specs, out_specs=out_specs, check_vma=False)
```
